16 devices in a mesh: dp: 2 (over y, z), tp: 8 (over x, core).
Axes of the slice: x: 4, y: 2, z: 1, core: 2. Of those that a mesh axis runs over, the one named last changes fastest.
The devices are a block of a 4x4x8 slice.
Arguments:
- x: bfloat16 [4096, 5120], P('dp'), parts along dimension 0
- w_gate: bfloat16 [5120, 16384], P(None, 'tp')
- w_up: bfloat16 [5120, 16384], P(None, 'tp')
- w_down: bfloat16 [16384, 5120], P('tp')
Outputs:
- output: bfloat16 [4096, 5120], P('dp'), parts along dimension 0
There are 2 independent parts. The reference program is written for one: setup_inputs(seed, part) draws one part's arguments, and reference() takes and returns one part's arrays. A program takes and returns all parts, laid end to end along the dimension named above; an argument that names none is the same for every part.
All inputs are finite; a program needn't handle non-finite values.
Results may differ from the reference program's by a relative error of at most 0.016.
Values are sent between devices in bfloat16 or wider.
A program may use at most 768 MiB of HBM per device.

```python
import jax
import jax.numpy as jnp

ROWS = 2048
D = 5120
FF = 16384


def setup_inputs(seed: int = 0, part: int = 0) -> dict:
    kx, kg, ku, kd = jax.random.split(jax.random.key(seed), 4)
    drawn = {
        "x": jax.random.normal(jax.random.fold_in(kx, part), (ROWS, D), jnp.float32),
        "w_gate": jax.random.normal(kg, (D, FF), jnp.float32) * D**-0.5,
        "w_up": jax.random.normal(ku, (D, FF), jnp.float32) * D**-0.5,
        "w_down": jax.random.normal(kd, (FF, D), jnp.float32) * FF**-0.5,
    }
    return {k: v.astype(jnp.bfloat16) for k, v in drawn.items()}


def reference(x, w_gate, w_up, w_down):
    gate = jnp.dot(x, w_gate, preferred_element_type=jnp.float32)
    up = jnp.dot(x, w_up, preferred_element_type=jnp.float32)
    hidden = (jax.nn.silu(gate) * up).astype(jnp.bfloat16)
    return jnp.dot(hidden, w_down, preferred_element_type=jnp.float32).astype(jnp.bfloat16)
```

```python
import functools

import jax
import jax.numpy as jnp
from jax import lax
from jax.experimental import pallas as pl
from jax.experimental.pallas import tpu as pltpu
from jax.sharding import PartitionSpec as P

F32 = jnp.float32
BF16 = jnp.bfloat16
CORES = 2
CHUNK = 256
STEPS = 4
SLOTS = 4


def kernel(
    n,
    x_ref, wg_ref, wu_ref, wd_ref,
    y_ref,
    xb, wg, wu, wd, hb, part, sib_s, sib_r, h1_s, h1_r, h2_s, h2_r, fin,
    x_sem, w_sem, wd_sem, sib_ss, sib_rs, h1_ss, h1_rs, h2_ss, h2_rs,
    a1_ss, a1_rs, a2_ss, a2_rs, fw_ss, fw_rs, loc_sem,
):
    chips = n // CORES
    rows, _ = x_ref.shape
    tile = wg.shape[-1]
    width = wd.shape[-1]
    half = CHUNK // CORES
    shard = half // chips
    piece = shard // 2
    chunks = rows // CHUNK
    units = chunks * STEPS

    me = lax.axis_index("tp")
    core = lax.rem(me, CORES)
    chip = me // CORES
    right_chip = lax.rem(chip + 1, chips)
    left_chip = lax.rem(chip + chips - 1, chips)
    far_chip = lax.rem(chip + 2, chips)
    right = right_chip * CORES + core
    left = left_chip * CORES + core
    sib = chip * CORES + (CORES - 1 - core)
    roles = (far_chip, left_chip, right_chip, chip)
    side = (right, left)

    def y_rows(u, owner_chip, owner_core, first=0, count=None):
        base = (u // STEPS) * CHUNK + owner_core * half + owner_chip * shard + first
        count = shard if count is None else count
        return pl.ds(pl.multiple_of(base, 16), count)

    def y_cols(u):
        return pl.ds(pl.multiple_of(lax.rem(u, STEPS) * width, 128), width)

    def slot_of(u):
        return lax.rem(u, SLOTS)

    def w_copies(s):
        k = lax.rem(s, 2)
        cols = pl.ds(pl.multiple_of(lax.rem(s, STEPS) * tile, 128), tile)
        return (
            pltpu.make_async_copy(wg_ref.at[:, cols], wg.at[k], w_sem.at[k, 0]),
            pltpu.make_async_copy(wu_ref.at[:, cols], wu.at[k], w_sem.at[k, 1]),
        )

    def wd_copy(j):
        cols = pl.ds(pl.multiple_of(j * width, 128), width)
        return pltpu.make_async_copy(wd_ref.at[:, cols], wd.at[j], wd_sem.at[j])

    def x_start(k):
        for h in range(CORES):
            owner_core = core if h == 1 else CORES - 1 - core
            for r, owner_chip in enumerate(roles):
                base = k * CHUNK + owner_core * half + owner_chip * shard
                pltpu.make_async_copy(
                    x_ref.at[pl.ds(pl.multiple_of(base, 16), shard)],
                    xb.at[lax.rem(k, 2), pl.ds(h * half + r * shard, shard)],
                    x_sem.at[lax.rem(k, 2)],
                ).start()

    def x_wait(k):
        pltpu.make_async_copy(
            x_ref.at[pl.ds(0, CHUNK)], xb.at[lax.rem(k, 2)], x_sem.at[lax.rem(k, 2)]
        ).wait()

    def remote(src, dst, ss, rs, dev):
        return pltpu.make_async_remote_copy(
            src_ref=src, dst_ref=dst, send_sem=ss, recv_sem=rs,
            device_id={"tp": dev}, device_id_type=pl.DeviceIdType.MESH,
        )

    def sib_copy(u):
        k = slot_of(u)
        return remote(sib_s.at[k], sib_r.at[k], sib_ss.at[k], sib_rs.at[k], sib)

    def h1_copy(u, d):
        k = slot_of(u)
        return remote(h1_s.at[k, d], h1_r.at[k, d], h1_ss.at[k, d], h1_rs.at[k, d], side[d])

    def h2_copy(u, d):
        k = slot_of(u)
        return remote(h2_s.at[k, d], h2_r.at[k, d], h2_ss.at[k, d], h2_rs.at[k, d], side[d])

    def a1_copy(u, d):
        k = slot_of(u)
        dst = y_ref.at[y_rows(u, chip, core), y_cols(u)]
        return remote(fin.at[k], dst, a1_ss.at[k, d], a1_rs.at[k, d], side[d])

    def a2_copy(u, d):
        k = slot_of(u)
        owner = (left_chip, right_chip)[d]
        at = y_ref.at[y_rows(u, owner, core, d * piece, piece), y_cols(u)]
        return remote(at, at, a2_ss.at[k, d], a2_rs.at[k, d], side[d])

    def fw_copy(u):
        k = slot_of(u)
        base = (u // STEPS) * CHUNK + core * half
        at = y_ref.at[pl.ds(pl.multiple_of(base, 16), half), y_cols(u)]
        return remote(at, at, fw_ss.at[k], fw_rs.at[k], sib)

    def loc_copy(u):
        k = slot_of(u)
        dst = y_ref.at[y_rows(u, chip, core), y_cols(u)]
        return pltpu.make_async_copy(fin.at[k], dst, loc_sem.at[k])

    barrier = pltpu.get_barrier_semaphore()
    for dev in (left, right, sib):
        pl.semaphore_signal(
            barrier, inc=1, device_id={"tp": dev}, device_id_type=pl.DeviceIdType.MESH
        )
    x_start(0)
    for c in w_copies(0):
        c.start()
    pl.semaphore_wait(barrier, 3)

    def load(ref, k, r, first=0, count=None):
        return ref[k, pl.ds(r * shard + first, shard if count is None else count)].astype(F32)

    def when(lo, s, hi):
        return pl.when(jnp.logical_and(s >= lo, s < hi))

    @pl.loop(0, units + STEPS + 5)
    def _(s):
        t = s - STEPS

        @pl.when(s < units)
        def _():
            k = s // STEPS

            @pl.when(lax.rem(s, STEPS) == 0)
            def _():
                x_wait(k)

                @pl.when(k + 1 < chunks)
                def _():
                    x_start(k + 1)

        @when(STEPS - 1, s, 2 * STEPS - 1)
        def _():
            wd_copy(s - (STEPS - 1)).start()

        @pl.when(s < units)
        def _():
            for c in w_copies(s):
                c.wait()

            @pl.when(s + 1 < units)
            def _():
                for c in w_copies(s + 1):
                    c.start()

        @when(0, t, units)
        def _():
            @pl.when(t < STEPS)
            def _():
                wd_copy(t).wait()

            k = slot_of(t)
            h = hb[lax.rem(t // STEPS, 2)]
            term = jnp.dot(h, wd[lax.rem(t, STEPS)], preferred_element_type=F32)
            sib_s[k] = term[:half].astype(BF16)
            part[k] = term[half:]
            sib_copy(t).start()

        @pl.when(s < units)
        def _():
            k = lax.rem(s, 2)
            b = lax.rem(s // STEPS, 2)
            xs = xb[b]
            gate = jnp.dot(xs, wg[k], preferred_element_type=F32)
            up = jnp.dot(xs, wu[k], preferred_element_type=F32)
            cols = pl.ds(pl.multiple_of(lax.rem(s, STEPS) * tile, 128), tile)
            hb[b, :, cols] = (jax.nn.silu(gate) * up).astype(BF16)

        @when(0, t, units)
        def _():
            sib_copy(t).wait()
            k = slot_of(t)
            for d in range(2):
                h1_s[k, d] = (
                    load(part, k, 0, d * piece, piece) + load(sib_r, k, 0, d * piece, piece)
                ).astype(BF16)
                h1_copy(t, d).start()

        @when(0, t - 1, units)
        def _():
            u = t - 1
            k = slot_of(u)
            for d in range(2):
                h1_copy(u, d).wait()
            for d in range(2):
                r = (2, 1)[d]
                for p in range(2):
                    v = load(part, k, r, p * piece, piece) + load(sib_r, k, r, p * piece, piece)
                    if p == d:
                        v = v + h1_r[k, d].astype(F32)
                    h2_s[k, d, pl.ds(p * piece, piece)] = v.astype(BF16)
                h2_copy(u, d).start()

        @when(0, t - 2, units)
        def _():
            u = t - 2
            k = slot_of(u)
            for d in range(2):
                h2_copy(u, d).wait()
            v = load(part, k, 3) + load(sib_r, k, 3)
            v = v + h2_r[k, 0].astype(F32) + h2_r[k, 1].astype(F32)
            fin[k] = v.astype(BF16)
            for d in range(2):
                a1_copy(u, d).start()
            loc_copy(u).start()

        @when(0, t - 3, units)
        def _():
            u = t - 3
            for d in range(2):
                a1_copy(u, d).wait()
            for d in range(2):
                a2_copy(u, d).start()
            loc_copy(u).wait()

        @when(0, t - 4, units)
        def _():
            u = t - 4
            for d in range(2):
                a2_copy(u, d).wait()
            fw_copy(u).start()

        @when(0, t - 5, units)
        def _():
            fw_copy(t - 5).wait()


def solution(mesh):
    n = mesh.shape["tp"]

    def step(x, w_gate, w_up, w_down):
        rows, d = x.shape
        f = w_gate.shape[1]
        tile = f // STEPS
        width = d // STEPS
        half = CHUNK // CORES
        shard = half // (n // CORES)
        piece = shard // 2
        dma = pltpu.SemaphoreType.DMA
        any_spec = pl.BlockSpec(memory_space=pltpu.HBM)
        return pl.pallas_call(
            functools.partial(kernel, n),
            out_shape=jax.ShapeDtypeStruct((rows, d), BF16),
            in_specs=[any_spec] * 4,
            out_specs=any_spec,
            scratch_shapes=[
                pltpu.VMEM((2, CHUNK, d), BF16),
                pltpu.VMEM((2, d, tile), BF16),
                pltpu.VMEM((2, d, tile), BF16),
                pltpu.VMEM((STEPS, f, width), BF16),
                pltpu.VMEM((2, CHUNK, f), BF16),
                pltpu.VMEM((SLOTS, half, width), F32),
                pltpu.VMEM((SLOTS, half, width), BF16),
                pltpu.VMEM((SLOTS, half, width), BF16),
                pltpu.VMEM((SLOTS, 2, piece, width), BF16),
                pltpu.VMEM((SLOTS, 2, piece, width), BF16),
                pltpu.VMEM((SLOTS, 2, shard, width), BF16),
                pltpu.VMEM((SLOTS, 2, shard, width), BF16),
                pltpu.VMEM((SLOTS, shard, width), BF16),
                dma((2,)),
                dma((2, 2)),
                dma((STEPS,)),
                dma((SLOTS,)),
                dma((SLOTS,)),
                dma((SLOTS, 2)),
                dma((SLOTS, 2)),
                dma((SLOTS, 2)),
                dma((SLOTS, 2)),
                dma((SLOTS, 2)),
                dma((SLOTS, 2)),
                dma((SLOTS, 2)),
                dma((SLOTS, 2)),
                dma((SLOTS,)),
                dma((SLOTS,)),
                dma((SLOTS,)),
            ],
            compiler_params=pltpu.CompilerParams(
                collective_id=0, has_side_effects=True, vmem_limit_bytes=67_043_328
            ),
            name="mlp_ring",
        )(x, w_gate, w_up, w_down)

    return jax.shard_map(
        step,
        mesh=mesh,
        in_specs=(P("dp", None), P(None, "tp"), P(None, "tp"), P("tp", None)),
        out_specs=P("dp", None),
        check_vma=False,
    )
```

```python
import functools

import jax
import jax.numpy as jnp
from jax import lax
from jax.experimental import pallas as pl
from jax.experimental.pallas import tpu as pltpu
from jax.sharding import PartitionSpec as P

F32 = jnp.float32
BF16 = jnp.bfloat16
CORES = 2
CHUNK = 256
UNITS = 4
TILES = 8
POINTS = UNITS + TILES
W_SLOTS = 4
LAG_FAR, LAG_NEAR, LAG_OWN, LAG_ON, LAG_SIB, LAG_END = 1, 5, 9, 13, 17, 21


def kernel(
    n,
    x_ref, wg_ref, wu_ref, wd_ref,
    y_ref, wd,
    xb, wb, hb, part, sib_s, sib_r, h1_s, h1_r, h2_s, h2_r, fin,
    x_sem, w_sem, wd_sem, sib_ss, sib_rs, h1_ss, h1_rs, h2_ss, h2_rs,
    a1_ss, a1_rs, a2_ss, a2_rs, fw_ss, fw_rs, loc_sem, in_sem,
):
    chips = n // CORES
    rows, _ = x_ref.shape
    tile = wb.shape[-1] // 2
    width = wd.shape[-1]
    half = CHUNK // CORES
    shard = half // chips
    piece = shard // 2
    chunks = rows // CHUNK

    me = lax.axis_index("tp")
    core = lax.rem(me, CORES)
    chip = me // CORES
    right_chip = lax.rem(chip + 1, chips)
    left_chip = lax.rem(chip + chips - 1, chips)
    far_chip = lax.rem(chip + 2, chips)
    sib = chip * CORES + (CORES - 1 - core)
    roles = (far_chip, left_chip, right_chip, chip)
    side = (right_chip * CORES + core, left_chip * CORES + core)

    def y_at(ref, k, i, owner_chip, first=0, count=None):
        base = k * CHUNK + core * half + owner_chip * shard + first
        count = shard if count is None else count
        return ref.at[i, pl.ds(pl.multiple_of(base, 16), count)]

    def by_chunk(k, body):
        @pl.when(k < chunks - 1)
        def _():
            body(y_ref)

        @pl.when(k == chunks - 1)
        def _():
            body(wd)

    def w_copies(w):
        k = w % W_SLOTS
        cols = pl.ds((w % TILES) * tile, tile)
        return (
            pltpu.make_async_copy(wg_ref.at[:, cols], wb.at[k, :, pl.ds(0, tile)], w_sem.at[k, 0]),
            pltpu.make_async_copy(wu_ref.at[:, cols], wb.at[k, :, pl.ds(tile, tile)], w_sem.at[k, 1]),
        )

    def w_start(w):
        for c in w_copies(w):
            c.start()

    def wd_copy(i):
        cols = pl.ds(i * width, width)
        return pltpu.make_async_copy(wd_ref.at[:, cols], wd.at[i], wd_sem.at[i])

    def x_start(k):
        for h in range(CORES):
            owner_core = core if h == 1 else CORES - 1 - core
            for r, owner_chip in enumerate(roles):
                base = k * CHUNK + owner_core * half + owner_chip * shard
                pltpu.make_async_copy(
                    x_ref.at[pl.ds(pl.multiple_of(base, 16), shard)],
                    xb.at[pl.ds(h * half + r * shard, shard)],
                    x_sem.at[0],
                ).start()

    def x_wait():
        pltpu.make_async_copy(x_ref.at[pl.ds(0, CHUNK)], xb, x_sem.at[0]).wait()

    def remote(src, dst, ss, rs, dev):
        return pltpu.make_async_remote_copy(
            src_ref=src, dst_ref=dst, send_sem=ss, recv_sem=rs,
            device_id={"tp": dev}, device_id_type=pl.DeviceIdType.MESH,
        )

    def sib_copy(i):
        return remote(sib_s.at[i], sib_r.at[i], sib_ss.at[i], sib_rs.at[i], sib)

    def h1_copy(i, d):
        return remote(h1_s.at[i, d], h1_r.at[i, d], h1_ss.at[i, d], h1_rs.at[i, d], side[d])

    def h2_copy(i, d):
        return remote(h2_s.at[i, d], h2_r.at[i, d], h2_ss.at[i, d], h2_rs.at[i, d], side[d])

    def a1_copy(ref, k, i, d):
        return remote(fin.at[i], y_at(ref, k, i, chip), a1_ss.at[i, d], a1_rs.at[i, d], side[d])

    def a2_copy(ref, k, i, d):
        at = y_at(ref, k, i, (left_chip, right_chip)[d], d * piece, piece)
        return remote(at, at, a2_ss.at[i, d], a2_rs.at[i, d], side[d])

    def fw_copy(ref, k, i):
        at = y_at(ref, k, i, 0, 0, half)
        p = lax.rem(k, 2)
        return remote(at, at, fw_ss.at[p, i], fw_rs.at[p, i], sib)

    def loc_copy(k, i):
        return pltpu.make_async_copy(fin.at[i], y_at(y_ref, k, i, chip), loc_sem.at[i])

    early = pl.ds(0, (chunks - 2) * CHUNK)
    late = pl.ds((chunks - 2) * CHUNK, CHUNK)

    def in_copy(i, at, p):
        return pltpu.make_async_copy(y_ref.at[i, at], wd.at[i, at], in_sem.at[p, i])

    barrier = pltpu.get_barrier_semaphore()
    for dev in (*side, sib):
        pl.semaphore_signal(
            barrier, inc=1, device_id={"tp": dev}, device_id_type=pl.DeviceIdType.MESH
        )
    x_start(0)
    for w in range(W_SLOTS - 1):
        w_start(w)
    pl.semaphore_wait(barrier, 3)

    def load(ref, i, r, first=0, count=None):
        return ref[i, pl.ds(r * shard + first, shard if count is None else count)].astype(F32)

    def point(k, c):
        if c < UNITS:
            @pl.when(jnp.logical_and(k >= 0, k < chunks))
            def _():
                @pl.when(k == 0)
                def _():
                    wd_copy(c).wait()

                if c == 0:

                    @pl.when(k + 1 < chunks)
                    def _():
                        x_start(k + 1)

                term = jnp.dot(hb[...], wd[c], preferred_element_type=F32)
                sib_s[c] = term[:half].astype(BF16)
                part[c] = term[half:]
                sib_copy(c).start()
        else:
            j = c - UNITS

            @pl.when(k + 1 < chunks)
            def _():
                if j == 0:
                    x_wait()
                for cp in w_copies(j):
                    cp.wait()
                if j == TILES - W_SLOTS + 1:

                    @pl.when(k < 0)
                    def _():
                        for i in range(UNITS):
                            wd_copy(i).start()

                if j < TILES - W_SLOTS + 1:
                    w_start(j + W_SLOTS - 1)
                else:

                    @pl.when(k + 2 < chunks)
                    def _():
                        w_start(j + W_SLOTS - 1)

                both = jnp.dot(xb[...], wb[j % W_SLOTS], preferred_element_type=F32)
                cols = pl.ds(j * tile, tile)
                hb[:, cols] = (jax.nn.silu(both[:, :tile]) * both[:, tile:]).astype(BF16)

        def stage(lag):
            i = (c - lag) % POINTS
            q = k + (c - lag) // POINTS

            def run(body):
                if i < UNITS:

                    @pl.when(jnp.logical_and(q >= 0, q < chunks))
                    def _():
                        body(q, i)

            return run

        @stage(LAG_FAR)
        def _(q, i):
            sib_copy(i).wait()
            for d in range(2):
                h1_s[i, d] = (
                    load(part, i, 0, d * piece, piece) + load(sib_r, i, 0, d * piece, piece)
                ).astype(BF16)
                h1_copy(i, d).start()
            for r in range(1, 4):
                part[i, pl.ds(r * shard, shard)] = load(part, i, r) + load(sib_r, i, r)

        @stage(LAG_NEAR)
        def _(q, i):
            for d in range(2):
                h1_copy(i, d).wait()
            for d in range(2):
                r = (2, 1)[d]
                h2_s[i, d, pl.ds(d * piece, piece)] = (
                    load(part, i, r, d * piece, piece) + h1_r[i, d].astype(F32)
                ).astype(BF16)
                h2_s[i, d, pl.ds((1 - d) * piece, piece)] = load(
                    part, i, r, (1 - d) * piece, piece
                ).astype(BF16)
                h2_copy(i, d).start()

        @stage(LAG_OWN)
        def _(q, i):
            for d in range(2):
                h2_copy(i, d).wait()
            v = load(part, i, 3) + h2_r[i, 0].astype(F32) + h2_r[i, 1].astype(F32)
            fin[i] = v.astype(BF16)

            def go(ref):
                for d in range(2):
                    a1_copy(ref, q, i, d).start()

            by_chunk(q, go)

            @pl.when(q < chunks - 1)
            def _():
                loc_copy(q, i).start()

            @pl.when(q == chunks - 1)
            def _():
                at = pl.ds(pl.multiple_of(q * CHUNK + core * half + chip * shard, 16), shard)
                wd[i, at] = v.astype(BF16)

        @stage(LAG_ON)
        def _(q, i):
            def go(ref):
                for d in range(2):
                    a1_copy(ref, q, i, d).wait()
                for d in range(2):
                    a2_copy(ref, q, i, d).start()

            by_chunk(q, go)

            @pl.when(q < chunks - 1)
            def _():
                loc_copy(q, i).wait()

        @stage(LAG_SIB)
        def _(q, i):
            def go(ref):
                for d in range(2):
                    a2_copy(ref, q, i, d).wait()
                fw_copy(ref, q, i).start()

            by_chunk(q, go)

        @stage(LAG_END)
        def _(q, i):
            by_chunk(q, lambda ref: fw_copy(ref, q, i).wait())

            @pl.when(q == chunks - 2)
            def _():
                in_copy(i, late, 1).start()

        if c == UNITS:
            @pl.when(k == chunks - 1)
            def _():
                for i in range(UNITS):
                    in_copy(i, early, 0).start()

    for c in range(UNITS, POINTS):
        point(jnp.int32(-1), c)

    @pl.loop(0, chunks + LAG_END // POINTS + 1)
    def _(k):
        for c in range(POINTS):
            point(k, c)

    for i in range(UNITS):
        in_copy(i, early, 0).wait()
        in_copy(i, late, 1).wait()


def write_out(v_ref, y_ref, sem):
    width = v_ref.shape[-1]
    copies = [
        pltpu.make_async_copy(v_ref.at[i], y_ref.at[:, pl.ds(i * width, width)], sem.at[i])
        for i in range(UNITS)
    ]
    for c in copies:
        c.start()
    for c in copies:
        c.wait()


def solution(mesh):
    n = mesh.shape["tp"]

    def step(x, w_gate, w_up, w_down):
        rows, d = x.shape
        f = w_gate.shape[1]
        tile = f // TILES
        width = d // UNITS
        half = CHUNK // CORES
        shard = half // (n // CORES)
        piece = shard // 2
        dma = pltpu.SemaphoreType.DMA
        hbm = pl.BlockSpec(memory_space=pltpu.HBM)
        vmem = pl.BlockSpec(memory_space=pltpu.VMEM)
        assert rows == f
        _, y = pl.pallas_call(
            functools.partial(kernel, n),
            out_shape=(
                jax.ShapeDtypeStruct((UNITS, rows, width), BF16),
                pltpu.VMEM((UNITS, f, width), BF16),
            ),
            in_specs=[hbm] * 4,
            out_specs=(hbm, vmem),
            scratch_shapes=[
                pltpu.VMEM((CHUNK, d), BF16),
                pltpu.VMEM((W_SLOTS, d, 2 * tile), BF16),
                pltpu.VMEM((CHUNK, f), BF16),
                pltpu.VMEM((UNITS, half, width), F32),
                pltpu.VMEM((UNITS, half, width), BF16),
                pltpu.VMEM((UNITS, half, width), BF16),
                pltpu.VMEM((UNITS, 2, piece, width), BF16),
                pltpu.VMEM((UNITS, 2, piece, width), BF16),
                pltpu.VMEM((UNITS, 2, shard, width), BF16),
                pltpu.VMEM((UNITS, 2, shard, width), BF16),
                pltpu.VMEM((UNITS, shard, width), BF16),
                dma((1,)),
                dma((W_SLOTS, 2)),
                dma((UNITS,)),
                dma((UNITS,)),
                dma((UNITS,)),
                *[dma((UNITS, 2))] * 8,
                dma((2, UNITS)),
                dma((2, UNITS)),
                dma((UNITS,)),
                dma((2, UNITS)),
            ],
            compiler_params=pltpu.CompilerParams(
                collective_id=0, has_side_effects=True, vmem_limit_bytes=42 << 20
            ),
            name="mlp_ring",
        )(x, w_gate, w_up, w_down)
        return pl.pallas_call(
            write_out,
            out_shape=jax.ShapeDtypeStruct((rows, d), BF16),
            in_specs=[vmem],
            out_specs=hbm,
            scratch_shapes=[dma((UNITS,))],
            compiler_params=pltpu.CompilerParams(vmem_limit_bytes=1 << 20),
            name="write_out",
        )(y)

    return jax.shard_map(
        step,
        mesh=mesh,
        in_specs=(P("dp", None), P(None, "tp"), P(None, "tp"), P("tp", None)),
        out_specs=P("dp", None),
        check_vma=False,
    )
```

```python
import functools

import jax
import jax.numpy as jnp
from jax import lax
from jax.experimental import pallas as pl
from jax.experimental.pallas import tpu as pltpu
from jax.sharding import PartitionSpec as P

F32 = jnp.float32
BF16 = jnp.bfloat16
CORES = 2
CHUNK = 256
UNITS = 4
TILES = 8
POINTS = UNITS + TILES
W_SLOTS = 4
LAG_FAR, LAG_NEAR, LAG_OWN, LAG_ON, LAG_SIB, LAG_END = (1, 1), (5, 5), (9, 9), (13, 13), (17, 17), (21, 21)


def kernel(
    n,
    x_ref, wg_ref, wu_ref, wd_ref,
    y_ref, wd,
    xb, wb, hb, part, sib_s, sib_r, h1_s, h1_r, h2_s, h2_r, fin,
    x_sem, w_sem, wd_sem, sib_ss, sib_rs, h1_ss, h1_rs, h2_ss, h2_rs,
    a1_ss, a1_rs, a2_ss, a2_rs, fw_ss, fw_rs, loc_sem, in_sem,
):
    chips = n // CORES
    rows, _ = x_ref.shape
    tile = wb.shape[-1] // 2
    width = wd.shape[-1]
    half = CHUNK // CORES
    shard = half // chips
    piece = shard // 2
    chunks = rows // CHUNK

    me = lax.axis_index("tp")
    core = lax.rem(me, CORES)
    chip = me // CORES
    right_chip = lax.rem(chip + 1, chips)
    left_chip = lax.rem(chip + chips - 1, chips)
    far_chip = lax.rem(chip + 2, chips)
    sib = chip * CORES + (CORES - 1 - core)
    roles = (far_chip, left_chip, right_chip, chip)
    side = (right_chip * CORES + core, left_chip * CORES + core)

    def y_at(ref, k, i, owner_chip, first=0, count=None):
        base = k * CHUNK + core * half + owner_chip * shard + first
        count = shard if count is None else count
        return ref.at[i, pl.ds(pl.multiple_of(base, 16), count)]

    def by_chunk(k, body):
        @pl.when(k < chunks - 1)
        def _():
            body(y_ref)

        @pl.when(k == chunks - 1)
        def _():
            body(wd)

    def w_copies(w):
        k = w % W_SLOTS
        cols = pl.ds((w % TILES) * tile, tile)
        return (
            pltpu.make_async_copy(wg_ref.at[:, cols], wb.at[k, :, pl.ds(0, tile)], w_sem.at[k, 0]),
            pltpu.make_async_copy(wu_ref.at[:, cols], wb.at[k, :, pl.ds(tile, tile)], w_sem.at[k, 1]),
        )

    def w_start(w):
        for c in w_copies(w):
            c.start()

    def wd_copy(i):
        cols = pl.ds(i * width, width)
        return pltpu.make_async_copy(wd_ref.at[:, cols], wd.at[i], wd_sem.at[i])

    def x_start(k):
        for h in range(CORES):
            owner_core = core if h == 1 else CORES - 1 - core
            for r, owner_chip in enumerate(roles):
                base = k * CHUNK + owner_core * half + owner_chip * shard
                pltpu.make_async_copy(
                    x_ref.at[pl.ds(pl.multiple_of(base, 16), shard)],
                    xb.at[pl.ds(h * half + r * shard, shard)],
                    x_sem.at[0],
                ).start()

    def x_wait():
        pltpu.make_async_copy(x_ref.at[pl.ds(0, CHUNK)], xb, x_sem.at[0]).wait()

    def remote(src, dst, ss, rs, dev):
        return pltpu.make_async_remote_copy(
            src_ref=src, dst_ref=dst, send_sem=ss, recv_sem=rs,
            device_id={"tp": dev}, device_id_type=pl.DeviceIdType.MESH,
        )

    def sib_copy(i):
        return remote(sib_s.at[i], sib_r.at[i], sib_ss.at[i], sib_rs.at[i], sib)

    def h1_copy(i, d):
        return remote(h1_s.at[i, d], h1_r.at[i, d], h1_ss.at[i, d], h1_rs.at[i, d], side[d])

    def h2_copy(i, d):
        return remote(h2_s.at[i, d], h2_r.at[i, d], h2_ss.at[i, d], h2_rs.at[i, d], side[d])

    def a1_copy(ref, k, i, d):
        return remote(fin.at[i], y_at(ref, k, i, chip), a1_ss.at[i, d], a1_rs.at[i, d], side[d])

    def a2_copy(ref, k, i, d):
        at = y_at(ref, k, i, (left_chip, right_chip)[d], d * piece, piece)
        return remote(at, at, a2_ss.at[i, d], a2_rs.at[i, d], side[d])

    def fw_copy(ref, k, i):
        at = y_at(ref, k, i, 0, 0, half)
        p = lax.rem(k, 2)
        return remote(at, at, fw_ss.at[p, i], fw_rs.at[p, i], sib)

    def loc_copy(k, i):
        return pltpu.make_async_copy(fin.at[i], y_at(y_ref, k, i, chip), loc_sem.at[i])

    early = pl.ds(0, (chunks - 2) * CHUNK)
    late = pl.ds((chunks - 2) * CHUNK, CHUNK)

    def in_copy(i, at, p):
        return pltpu.make_async_copy(y_ref.at[i, at], wd.at[i, at], in_sem.at[p, i])

    barrier = pltpu.get_barrier_semaphore()
    for dev in (*side, sib):
        pl.semaphore_signal(
            barrier, inc=1, device_id={"tp": dev}, device_id_type=pl.DeviceIdType.MESH
        )
    x_start(0)
    w_start(0)
    x_wait()
    w_start(1)
    w_start(2)

    def load(ref, i, r, first=0, count=None):
        return ref[i, pl.ds(r * shard + first, shard if count is None else count)].astype(F32)

    def when(cond):
        if isinstance(cond, bool):
            return (lambda body: body()) if cond else (lambda body: None)
        return pl.when(cond)

    def within(lo, q, hi):
        if isinstance(q, int):
            return False if q < lo else q < hi
        return jnp.logical_and(q >= lo, q < hi)

    def point(k, c):
        if c < UNITS:
            @when(within(0, k, chunks))
            def _():
                @when(k == 0)
                def _():
                    wd_copy(c).wait()
                    if c + 3 < UNITS:
                        wd_copy(c + 3).start()
                    else:
                        w_start(TILES + c + 3 - UNITS)

                if c == 0:

                    @when(k + 1 < chunks)
                    def _():
                        x_start(k + 1)

                term = jnp.dot(hb[...], wd[c], preferred_element_type=F32)
                sib_s[c] = term[:half].astype(BF16)
                part[c] = term[half:]
                sib_copy(c).start()
        else:
            j = c - UNITS

            @when(k + 1 < chunks)
            def _():
                if j == 0:

                    @when(k >= 0)
                    def _():
                        x_wait()

                for cp in w_copies(j):
                    cp.wait()

                @when(k < 0)
                def _():
                    if j + 3 < TILES:
                        w_start(j + 3)
                    else:
                        wd_copy(j + 3 - TILES).start()

                ahead = j + W_SLOTS - 1
                if ahead < TILES:

                    @when(k >= 0)
                    def _():
                        w_start(ahead)
                else:

                    @when(within(0, k, chunks - 2))
                    def _():
                        w_start(ahead)

                both = jnp.dot(xb[...], wb[j % W_SLOTS], preferred_element_type=F32)
                cols = pl.ds(j * tile, tile)
                hb[:, cols] = (jax.nn.silu(both[:, :tile]) * both[:, tile:]).astype(BF16)

        def stage(lag, first):
            def run(body):
                for points, early_unit in ((first, True), (lag, False)):
                    i = (c - points) % POINTS
                    q = k + (c - points) // POINTS
                    if i >= UNITS:
                        continue
                    if first == lag:
                        on = within(0, q, chunks)
                        if early_unit:
                            continue
                    elif early_unit:
                        on = q == 0
                    else:
                        on = within(1, q, chunks)

                    @when(on)
                    def _():
                        body(q, i)

            return run

        @stage(*LAG_FAR)
        def _(q, i):
            sib_copy(i).wait()
            for d in range(2):
                h1_s[i, d] = (
                    load(part, i, 0, d * piece, piece) + load(sib_r, i, 0, d * piece, piece)
                ).astype(BF16)
                h1_copy(i, d).start()
            for r in range(1, 4):
                part[i, pl.ds(r * shard, shard)] = load(part, i, r) + load(sib_r, i, r)

        @stage(*LAG_NEAR)
        def _(q, i):
            for d in range(2):
                h1_copy(i, d).wait()
            for d in range(2):
                r = (2, 1)[d]
                h2_s[i, d, pl.ds(d * piece, piece)] = (
                    load(part, i, r, d * piece, piece) + h1_r[i, d].astype(F32)
                ).astype(BF16)
                h2_s[i, d, pl.ds((1 - d) * piece, piece)] = load(
                    part, i, r, (1 - d) * piece, piece
                ).astype(BF16)
                h2_copy(i, d).start()

        @stage(*LAG_OWN)
        def _(q, i):
            for d in range(2):
                h2_copy(i, d).wait()
            v = load(part, i, 3) + h2_r[i, 0].astype(F32) + h2_r[i, 1].astype(F32)
            fin[i] = v.astype(BF16)

            def go(ref):
                for d in range(2):
                    a1_copy(ref, q, i, d).start()

            by_chunk(q, go)

            @when(q < chunks - 1)
            def _():
                loc_copy(q, i).start()

            @when(q == chunks - 1)
            def _():
                at = pl.ds(pl.multiple_of(q * CHUNK + core * half + chip * shard, 16), shard)
                wd[i, at] = v.astype(BF16)

        @stage(*LAG_ON)
        def _(q, i):
            def go(ref):
                for d in range(2):
                    a1_copy(ref, q, i, d).wait()
                for d in range(2):
                    a2_copy(ref, q, i, d).start()

            by_chunk(q, go)

            @when(q < chunks - 1)
            def _():
                loc_copy(q, i).wait()

        @stage(*LAG_SIB)
        def _(q, i):
            def go(ref):
                for d in range(2):
                    a2_copy(ref, q, i, d).wait()
                fw_copy(ref, q, i).start()

            by_chunk(q, go)

        @stage(*LAG_END)
        def _(q, i):
            by_chunk(q, lambda ref: fw_copy(ref, q, i).wait())

            @when(q == chunks - 2)
            def _():
                in_copy(i, late, 1).start()

        if c == UNITS:
            @when(k == chunks - 1)
            def _():
                for i in range(UNITS):
                    in_copy(i, early, 0).start()

    for c in range(UNITS, POINTS):
        point(-1, c)

    pl.semaphore_wait(barrier, 3)

    @pl.loop(0, chunks + LAG_END[0] // POINTS + 1)
    def _(k):
        for c in range(POINTS):
            point(k, c)

    for i in range(UNITS):
        in_copy(i, early, 0).wait()
        in_copy(i, late, 1).wait()


def write_out(v_ref, y_ref, sem):
    width = v_ref.shape[-1]
    copies = [
        pltpu.make_async_copy(v_ref.at[i], y_ref.at[:, pl.ds(i * width, width)], sem.at[i])
        for i in range(UNITS)
    ]
    for c in copies:
        c.start()
    for c in copies:
        c.wait()


def solution(mesh):
    n = mesh.shape["tp"]

    def step(x, w_gate, w_up, w_down):
        rows, d = x.shape
        f = w_gate.shape[1]
        tile = f // TILES
        width = d // UNITS
        half = CHUNK // CORES
        shard = half // (n // CORES)
        piece = shard // 2
        dma = pltpu.SemaphoreType.DMA
        hbm = pl.BlockSpec(memory_space=pltpu.HBM)
        vmem = pl.BlockSpec(memory_space=pltpu.VMEM)
        assert rows == f
        _, y = pl.pallas_call(
            functools.partial(kernel, n),
            out_shape=(
                jax.ShapeDtypeStruct((UNITS, rows, width), BF16),
                pltpu.VMEM((UNITS, f, width), BF16),
            ),
            in_specs=[hbm] * 4,
            out_specs=(hbm, vmem),
            scratch_shapes=[
                pltpu.VMEM((CHUNK, d), BF16),
                pltpu.VMEM((W_SLOTS, d, 2 * tile), BF16),
                pltpu.VMEM((CHUNK, f), BF16),
                pltpu.VMEM((UNITS, half, width), F32),
                pltpu.VMEM((UNITS, half, width), BF16),
                pltpu.VMEM((UNITS, half, width), BF16),
                pltpu.VMEM((UNITS, 2, piece, width), BF16),
                pltpu.VMEM((UNITS, 2, piece, width), BF16),
                pltpu.VMEM((UNITS, 2, shard, width), BF16),
                pltpu.VMEM((UNITS, 2, shard, width), BF16),
                pltpu.VMEM((UNITS, shard, width), BF16),
                dma((1,)),
                dma((W_SLOTS, 2)),
                dma((UNITS,)),
                dma((UNITS,)),
                dma((UNITS,)),
                *[dma((UNITS, 2))] * 8,
                dma((2, UNITS)),
                dma((2, UNITS)),
                dma((UNITS,)),
                dma((2, UNITS)),
            ],
            compiler_params=pltpu.CompilerParams(
                collective_id=0, has_side_effects=True, vmem_limit_bytes=42 << 20
            ),
            name="mlp_ring",
        )(x, w_gate, w_up, w_down)
        return pl.pallas_call(
            write_out,
            out_shape=jax.ShapeDtypeStruct((rows, d), BF16),
            in_specs=[vmem],
            out_specs=hbm,
            scratch_shapes=[dma((UNITS,))],
            compiler_params=pltpu.CompilerParams(vmem_limit_bytes=1 << 20),
            name="write_out",
        )(y)

    return jax.shard_map(
        step,
        mesh=mesh,
        in_specs=(P("dp", None), P(None, "tp"), P(None, "tp"), P("tp", None)),
        out_specs=P("dp", None),
        check_vma=False,
    )
```

```python
import functools

import jax
import jax.numpy as jnp
from jax import lax
from jax.experimental import pallas as pl
from jax.experimental.pallas import tpu as pltpu
from jax.sharding import PartitionSpec as P

F32 = jnp.float32
BF16 = jnp.bfloat16
CORES = 2
CHUNK = 256
UNITS = 4
TILES = 8
POINTS = UNITS + TILES
W_SLOTS = 4
LAG_FAR, LAG_NEAR, LAG_OWN, LAG_ON, LAG_SIB, LAG_END = (1, 1), (5, 4), (9, 8), (13, 12), (17, 17), (21, 21)


def kernel(
    n,
    x_ref, wg_ref, wu_ref, wd_ref,
    y_ref, wd,
    xb, wb, hb, part, sib_s, sib_r, h1_s, h1_r, h2_s, h2_r, fin,
    x_sem, w_sem, wd_sem, sib_ss, sib_rs, h1_ss, h1_rs, h2_ss, h2_rs,
    a1_ss, a1_rs, a2_ss, a2_rs, fw_ss, fw_rs, loc_sem, in_sem,
):
    chips = n // CORES
    rows, _ = x_ref.shape
    tile = wb.shape[-1] // 2
    width = wd.shape[-1]
    half = CHUNK // CORES
    shard = half // chips
    piece = shard // 2
    chunks = rows // CHUNK

    me = lax.axis_index("tp")
    core = lax.rem(me, CORES)
    chip = me // CORES
    right_chip = lax.rem(chip + 1, chips)
    left_chip = lax.rem(chip + chips - 1, chips)
    far_chip = lax.rem(chip + 2, chips)
    sib = chip * CORES + (CORES - 1 - core)
    roles = (far_chip, left_chip, right_chip, chip)
    side = (right_chip * CORES + core, left_chip * CORES + core)

    def y_at(ref, k, i, owner_chip, first=0, count=None):
        base = k * CHUNK + core * half + owner_chip * shard + first
        count = shard if count is None else count
        return ref.at[i, pl.ds(pl.multiple_of(base, 16), count)]

    def by_chunk(k, body):
        @pl.when(k < chunks - 1)
        def _():
            body(y_ref)

        @pl.when(k == chunks - 1)
        def _():
            body(wd)

    def w_copies(w):
        k = w % W_SLOTS
        cols = pl.ds((w % TILES) * tile, tile)
        return (
            pltpu.make_async_copy(wg_ref.at[:, cols], wb.at[k, :, pl.ds(0, tile)], w_sem.at[k, 0]),
            pltpu.make_async_copy(wu_ref.at[:, cols], wb.at[k, :, pl.ds(tile, tile)], w_sem.at[k, 1]),
        )

    def w_start(w):
        for c in w_copies(w):
            c.start()

    def wd_copy(i):
        cols = pl.ds(i * width, width)
        return pltpu.make_async_copy(wd_ref.at[:, cols], wd.at[i], wd_sem.at[i])

    def x_start(k):
        for h in range(CORES):
            owner_core = core if h == 1 else CORES - 1 - core
            for r, owner_chip in enumerate(roles):
                base = k * CHUNK + owner_core * half + owner_chip * shard
                pltpu.make_async_copy(
                    x_ref.at[pl.ds(pl.multiple_of(base, 16), shard)],
                    xb.at[pl.ds(h * half + r * shard, shard)],
                    x_sem.at[0],
                ).start()

    def x_wait():
        pltpu.make_async_copy(x_ref.at[pl.ds(0, CHUNK)], xb, x_sem.at[0]).wait()

    def remote(src, dst, ss, rs, dev):
        return pltpu.make_async_remote_copy(
            src_ref=src, dst_ref=dst, send_sem=ss, recv_sem=rs,
            device_id={"tp": dev}, device_id_type=pl.DeviceIdType.MESH,
        )

    def sib_copy(i):
        return remote(sib_s.at[i], sib_r.at[i], sib_ss.at[i], sib_rs.at[i], sib)

    def h1_copy(i, d):
        return remote(h1_s.at[i, d], h1_r.at[i, d], h1_ss.at[i, d], h1_rs.at[i, d], side[d])

    def h2_copy(i, d):
        return remote(h2_s.at[i, d], h2_r.at[i, d], h2_ss.at[i, d], h2_rs.at[i, d], side[d])

    def a1_copy(ref, k, i, d):
        return remote(fin.at[i], y_at(ref, k, i, chip), a1_ss.at[i, d], a1_rs.at[i, d], side[d])

    def a2_copy(ref, k, i, d):
        at = y_at(ref, k, i, (left_chip, right_chip)[d], d * piece, piece)
        return remote(at, at, a2_ss.at[i, d], a2_rs.at[i, d], side[d])

    def fw_copy(ref, k, i):
        at = y_at(ref, k, i, 0, 0, half)
        p = lax.rem(k, 2)
        return remote(at, at, fw_ss.at[p, i], fw_rs.at[p, i], sib)

    def loc_copy(k, i):
        return pltpu.make_async_copy(fin.at[i], y_at(y_ref, k, i, chip), loc_sem.at[i])

    early = pl.ds(0, (chunks - 2) * CHUNK)
    late = pl.ds((chunks - 2) * CHUNK, CHUNK)

    def in_copy(i, at, p):
        return pltpu.make_async_copy(y_ref.at[i, at], wd.at[i, at], in_sem.at[p, i])

    barrier = pltpu.get_barrier_semaphore()
    for dev in (*side, sib):
        pl.semaphore_signal(
            barrier, inc=1, device_id={"tp": dev}, device_id_type=pl.DeviceIdType.MESH
        )
    x_start(0)
    w_start(0)
    x_wait()
    w_start(1)
    w_start(2)

    def load(ref, i, r, first=0, count=None):
        return ref[i, pl.ds(r * shard + first, shard if count is None else count)].astype(F32)

    def when(cond):
        if isinstance(cond, bool):
            return (lambda body: body()) if cond else (lambda body: None)
        return pl.when(cond)

    def within(lo, q, hi):
        if isinstance(q, int):
            return False if q < lo else q < hi
        return jnp.logical_and(q >= lo, q < hi)

    def point(k, c):
        if c < UNITS:
            @when(within(0, k, chunks))
            def _():
                @when(k == 0)
                def _():
                    wd_copy(c).wait()
                    if c + 3 < UNITS:
                        wd_copy(c + 3).start()
                    else:
                        w_start(TILES + c + 3 - UNITS)

                if c == 0:

                    @when(k + 1 < chunks)
                    def _():
                        x_start(k + 1)

                term = jnp.dot(hb[...], wd[c], preferred_element_type=F32)
                sib_s[c] = term[:half].astype(BF16)
                part[c] = term[half:]
                sib_copy(c).start()
        else:
            j = c - UNITS

            @when(k + 1 < chunks)
            def _():
                if j == 0:

                    @when(k >= 0)
                    def _():
                        x_wait()

                for cp in w_copies(j):
                    cp.wait()

                @when(k < 0)
                def _():
                    if j + 3 < TILES:
                        w_start(j + 3)
                    else:
                        wd_copy(j + 3 - TILES).start()

                ahead = j + W_SLOTS - 1
                if ahead < TILES:

                    @when(k >= 0)
                    def _():
                        w_start(ahead)
                else:

                    @when(within(0, k, chunks - 2))
                    def _():
                        w_start(ahead)

                both = jnp.dot(xb[...], wb[j % W_SLOTS], preferred_element_type=F32)
                cols = pl.ds(j * tile, tile)
                hb[:, cols] = (jax.nn.silu(both[:, :tile]) * both[:, tile:]).astype(BF16)

        def stage(lag, first):
            def run(body):
                for points, early_unit in ((first, True), (lag, False)):
                    i = (c - points) % POINTS
                    q = k + (c - points) // POINTS
                    if i >= UNITS:
                        continue
                    if first == lag:
                        on = within(0, q, chunks)
                        if early_unit:
                            continue
                    elif early_unit:
                        on = q == 0
                    else:
                        on = within(1, q, chunks)

                    @when(on)
                    def _():
                        body(q, i)

            return run

        @stage(*LAG_FAR)
        def _(q, i):
            sib_copy(i).wait()
            for d in range(2):
                h1_s[i, d] = (
                    load(part, i, 0, d * piece, piece) + load(sib_r, i, 0, d * piece, piece)
                ).astype(BF16)
                h1_copy(i, d).start()
            for r in range(1, 4):
                part[i, pl.ds(r * shard, shard)] = load(part, i, r) + load(sib_r, i, r)

        @stage(*LAG_NEAR)
        def _(q, i):
            for d in range(2):
                h1_copy(i, d).wait()
            for d in range(2):
                r = (2, 1)[d]
                h2_s[i, d, pl.ds(d * piece, piece)] = (
                    load(part, i, r, d * piece, piece) + h1_r[i, d].astype(F32)
                ).astype(BF16)
                h2_s[i, d, pl.ds((1 - d) * piece, piece)] = load(
                    part, i, r, (1 - d) * piece, piece
                ).astype(BF16)
                h2_copy(i, d).start()

        @stage(*LAG_OWN)
        def _(q, i):
            for d in range(2):
                h2_copy(i, d).wait()
            v = load(part, i, 3) + h2_r[i, 0].astype(F32) + h2_r[i, 1].astype(F32)
            fin[i] = v.astype(BF16)

            def go(ref):
                for d in range(2):
                    a1_copy(ref, q, i, d).start()

            by_chunk(q, go)

            @when(q < chunks - 1)
            def _():
                loc_copy(q, i).start()

            @when(q == chunks - 1)
            def _():
                at = pl.ds(pl.multiple_of(q * CHUNK + core * half + chip * shard, 16), shard)
                wd[i, at] = v.astype(BF16)

        @stage(*LAG_ON)
        def _(q, i):
            def go(ref):
                for d in range(2):
                    a1_copy(ref, q, i, d).wait()
                for d in range(2):
                    a2_copy(ref, q, i, d).start()

            by_chunk(q, go)

            @when(q < chunks - 1)
            def _():
                loc_copy(q, i).wait()

        @stage(*LAG_SIB)
        def _(q, i):
            def go(ref):
                for d in range(2):
                    a2_copy(ref, q, i, d).wait()
                fw_copy(ref, q, i).start()

            by_chunk(q, go)

        @stage(*LAG_END)
        def _(q, i):
            by_chunk(q, lambda ref: fw_copy(ref, q, i).wait())

            @when(q == chunks - 2)
            def _():
                in_copy(i, late, 1).start()

        if c == UNITS:
            @when(k == chunks - 1)
            def _():
                for i in range(UNITS):
                    in_copy(i, early, 0).start()

    for c in range(UNITS, POINTS):
        point(-1, c)

    pl.semaphore_wait(barrier, 3)

    @pl.loop(0, chunks + LAG_END[0] // POINTS + 1)
    def _(k):
        for c in range(POINTS):
            point(k, c)

    for i in range(UNITS):
        in_copy(i, early, 0).wait()
        in_copy(i, late, 1).wait()


def write_out(v_ref, y_ref, sem):
    width = v_ref.shape[-1]
    copies = [
        pltpu.make_async_copy(v_ref.at[i], y_ref.at[:, pl.ds(i * width, width)], sem.at[i])
        for i in range(UNITS)
    ]
    for c in copies:
        c.start()
    for c in copies:
        c.wait()


def solution(mesh):
    n = mesh.shape["tp"]

    def step(x, w_gate, w_up, w_down):
        rows, d = x.shape
        f = w_gate.shape[1]
        tile = f // TILES
        width = d // UNITS
        half = CHUNK // CORES
        shard = half // (n // CORES)
        piece = shard // 2
        dma = pltpu.SemaphoreType.DMA
        hbm = pl.BlockSpec(memory_space=pltpu.HBM)
        vmem = pl.BlockSpec(memory_space=pltpu.VMEM)
        assert rows == f
        _, y = pl.pallas_call(
            functools.partial(kernel, n),
            out_shape=(
                jax.ShapeDtypeStruct((UNITS, rows, width), BF16),
                pltpu.VMEM((UNITS, f, width), BF16),
            ),
            in_specs=[hbm] * 4,
            out_specs=(hbm, vmem),
            scratch_shapes=[
                pltpu.VMEM((CHUNK, d), BF16),
                pltpu.VMEM((W_SLOTS, d, 2 * tile), BF16),
                pltpu.VMEM((CHUNK, f), BF16),
                pltpu.VMEM((UNITS, half, width), F32),
                pltpu.VMEM((UNITS, half, width), BF16),
                pltpu.VMEM((UNITS, half, width), BF16),
                pltpu.VMEM((UNITS, 2, piece, width), BF16),
                pltpu.VMEM((UNITS, 2, piece, width), BF16),
                pltpu.VMEM((UNITS, 2, shard, width), BF16),
                pltpu.VMEM((UNITS, 2, shard, width), BF16),
                pltpu.VMEM((UNITS, shard, width), BF16),
                dma((1,)),
                dma((W_SLOTS, 2)),
                dma((UNITS,)),
                dma((UNITS,)),
                dma((UNITS,)),
                *[dma((UNITS, 2))] * 8,
                dma((2, UNITS)),
                dma((2, UNITS)),
                dma((UNITS,)),
                dma((2, UNITS)),
            ],
            compiler_params=pltpu.CompilerParams(
                collective_id=0, has_side_effects=True, vmem_limit_bytes=42 << 20
            ),
            name="mlp_ring",
        )(x, w_gate, w_up, w_down)
        return pl.pallas_call(
            write_out,
            out_shape=jax.ShapeDtypeStruct((rows, d), BF16),
            in_specs=[vmem],
            out_specs=hbm,
            scratch_shapes=[dma((UNITS,))],
            compiler_params=pltpu.CompilerParams(vmem_limit_bytes=1 << 20),
            name="write_out",
        )(y)

    return jax.shard_map(
        step,
        mesh=mesh,
        in_specs=(P("dp", None), P(None, "tp"), P(None, "tp"), P("tp", None)),
        out_specs=P("dp", None),
        check_vma=False,
    )
```
